32 devices in a mesh: train: 2 (over y), tp: 8 (over z, x), dp: 2 (over core).
Axes of the slice: x: 2, y: 2, z: 4, core: 2. Of those that a mesh axis runs over, the one named last changes fastest.
Arguments:
- adapter_down_factor: bfloat16 [2, 2, 64, 8192], P(None, None, None, ('train', 'tp')), may hold values from -6 to 6
- adapter_up_factor: bfloat16 [2, 2, 1024, 64], P(None, None, ('train', 'tp')), may hold values from -0.75 to 0.75
- projection_weight: bfloat16 [2, 2, 1024, 8192], P(None, None, 'tp'), may hold values from -6 to 6
Outputs:
- merged: bfloat16 [2, 2, 1024, 8192], P(None, None, 'tp')
The draws below stay inside these ranges and needn't reach their ends.
All inputs are finite; a program needn't handle non-finite values.
Results may differ from the reference program's by a relative error of at most 0.001.
Values may be sent and summed in bfloat16 or wider, within the bound.
A program may use at most 64 MiB of HBM per device.

```python
import jax
import jax.numpy as jnp

MODEL_WIDTH = 8192
KEY_ROWS = 1024
ADAPTER_RANK = 64
DECODER_LAYERS = 2


def level_of(rng, dims, cuts, low, top_value):
    def one(position, parts):
        steps = jax.random.uniform(jax.random.fold_in(jax.random.fold_in(rng, 6), position), (parts,), jnp.float32, low / len(cuts), top_value / len(cuts))
        return jnp.repeat(jnp.exp(steps), dims[position] // parts).reshape((-1,) + (1,) * (len(dims) - position - 1))

    factor_of = one(*cuts[0])
    for cut in cuts[1:]:
        factor_of = factor_of * one(*cut)
    return factor_of


def centred(own_key, dims, scale, most, cuts=(), dtype=jnp.bfloat16):
    entries = jax.random.normal(own_key, dims, jnp.float32) * scale
    if len(cuts) > 0:
        entries = level_of(own_key, dims, cuts, -0.22, 0.18) * entries
    return jnp.clip(entries, min=-most, max=most).astype(dtype)


def setup_inputs(seed: int = 0) -> dict:
    seeds = jax.random.split(jax.random.key(seed), 4)
    adapter_down_factor = centred(seeds[0], (DECODER_LAYERS, 2, ADAPTER_RANK, MODEL_WIDTH), 1.0, 6.0, ((3, 16),))
    adapter_up_factor = centred(seeds[1], (DECODER_LAYERS, 2, KEY_ROWS, ADAPTER_RANK), 0.125, 0.75, ((2, 16),))
    projection_weight = centred(seeds[2], (DECODER_LAYERS, 2, KEY_ROWS, MODEL_WIDTH), 1.0, 6.0, ((2, 8),))
    return dict(adapter_down_factor=adapter_down_factor, adapter_up_factor=adapter_up_factor, projection_weight=projection_weight)


adapter_scale = 2.0


def reference(adapter_down_factor, adapter_up_factor, projection_weight):
    weight_update = jnp.einsum("eitd,eidh->eith", adapter_up_factor.astype(jnp.float32), adapter_down_factor.astype(jnp.float32))
    return (projection_weight.astype(jnp.float32) + adapter_scale * weight_update).astype(jnp.bfloat16)
```

```python
import functools

import jax
import jax.numpy as jnp
from jax import lax
from jax.experimental import pallas as pl
from jax.experimental.pallas import tpu as pltpu
from jax.sharding import PartitionSpec as P

adapter_scale = 2.0
MESH = pl.DeviceIdType.MESH


def place(train, tp, dp):
    return {"train": train, "tp": tp, "dp": dp}


def nearest(z, depth, j):
    if j == 0:
        return z
    low = jnp.minimum(z, depth - 1 - z)
    side = jnp.where(2 * z < depth - 1, 1, -1)
    near = z + side * ((j + 1) // 2) * (1 if j % 2 else -1)
    far = z + side * (j - low)
    return jnp.where(j <= 2 * low, near, far)


def gather_merge(
    tp, train, layers, kinds,
    down_ref, up_ref, weight_ref, out_ref,
    downs, ups, recv_sem, pass_recv, link_sem, line_sem, pass_sem, up_send, up_recv, weight_sem,
):
    y = lax.axis_index("train")
    t = lax.axis_index("tp")
    core = lax.axis_index("dp")
    depth = tp // 2
    z, x = t // 2, t % 2
    columns = down_ref.shape[-1]
    up_rows = up_ref.shape[2]
    other = 1 - core

    weight_copy = pltpu.make_async_copy(weight_ref, out_ref, weight_sem)
    weight_copy.start()

    def device(yy, zz, xx):
        return place(yy, zz * 2 + xx, core)

    to_x = device(y, z, 1 - x)
    to_y = device(1 - y, z, x)
    partner = place(y, t, other)

    group = y * tp + t
    up_target = group // train
    up_slot = group % train

    barrier = pltpu.get_barrier_semaphore()

    def greet(where):
        pl.semaphore_signal(barrier, inc=1, device_id=where, device_id_type=MESH)

    greet(to_x)
    greet(to_y)
    greet(partner)

    @pl.when(z > 0)
    def _():
        greet(device(y, z - 1, x))

    @pl.when(z < depth - 1)
    def _():
        greet(device(y, z + 1, x))

    for j in range(train):
        source = t * train + j

        @pl.when(source != group)
        def _():
            greet(place(source // tp, source % tp, core))

    peers = 3 + jnp.where(z > 0, 1, 0) + jnp.where(z < depth - 1, 1, 0)
    for yy in range(train):
        peers += jnp.where(yy * tp + up_target != group, 1, 0)
    pl.semaphore_wait(barrier, peers)

    def up_copy(yy):
        return pltpu.make_async_remote_copy(
            src_ref=up_ref, dst_ref=ups.at[up_slot],
            send_sem=up_send.at[yy], recv_sem=up_recv.at[up_slot],
            device_id=place(yy, up_target, core), device_id_type=MESH,
        )

    def index(yy, zz, xx, e, kind):
        return ((yy * tp + zz * 2 + xx) * layers + e) * kinds + kind

    def send(src, piece, where, sem):
        pltpu.make_async_remote_copy(
            src_ref=src, dst_ref=downs.at[piece], send_sem=sem,
            recv_sem=recv_sem.at[piece // (layers * kinds) * kinds + piece % kinds],
            device_id=where, device_id_type=MESH,
        ).start()

    def hand_over(piece):
        pltpu.make_async_remote_copy(
            src_ref=downs.at[piece], dst_ref=downs.at[piece], send_sem=pass_sem,
            recv_sem=pass_recv.at[piece // (layers * kinds) * kinds + piece % kinds],
            device_id=partner, device_id_type=MESH,
        ).start()

    def arrive(piece):
        sem = recv_sem.at[piece // (layers * kinds) * kinds + piece % kinds]
        pltpu.make_async_copy(downs.at[piece], downs.at[piece], sem).wait()

    x_sem, y_sem = link_sem.at[0], link_sem.at[1]

    for kind in range(kinds):
        piece = index(y, z, x, core, kind)
        mine = down_ref.at[core, kind]

        @pl.when(z > 0)
        def _():
            send(mine, piece, device(y, z - 1, x), line_sem.at[kind, z])

        @pl.when(z < depth - 1)
        def _():
            send(mine, piece, device(y, z + 1, x), line_sem.at[kind, depth])

        send(mine, piece, to_x, x_sem)
        send(mine, piece, to_y, y_sem)

    for yy in range(train):
        @pl.when(yy * tp + up_target != group)
        def _():
            up_copy(yy).start()

    for e in range(layers):
        for kind in range(kinds):
            downs[index(y, z, x, e, kind)] = down_ref[e, kind]

    def combine(yy, zz, xx, e, kind):
        block = downs[index(yy, zz, xx, e, kind)]
        at = pl.ds(pl.multiple_of((yy * tp + zz * 2 + xx) * columns, columns), columns)
        for j in range(train):
            rows = pl.ds(j * up_rows, up_rows)
            update = jnp.dot(
                ups[j, e, kind] * adapter_scale, block, preferred_element_type=jnp.float32
            )
            old = out_ref[e, kind, rows, at].astype(jnp.float32)
            out_ref[e, kind, rows, at] = (old + update).astype(out_ref.dtype)

    def merge(level):
        zz = nearest(z, depth, level)
        for yy in (y, 1 - y):
            for xx in (x, 1 - x):
                if level == 0 and yy is y and xx is x:
                    continue
                for kind in range(kinds):
                    piece = index(yy, zz, xx, other, kind)
                    sem = pass_recv.at[piece // (layers * kinds) * kinds + piece % kinds]
                    pltpu.make_async_copy(downs.at[piece], downs.at[piece], sem).wait()

        def step(i, carry):
            kind = i % kinds
            e = i // kinds % layers
            corner = i // (kinds * layers)
            combine(corner // 2, zz, corner % 2, e, kind)
            return carry

        lax.fori_loop(0, 4 * layers * kinds, step, 0)

    for step in range(depth + 3):
        for kind in range(kinds):
            first, second = (to_x, to_y) if kind == 0 else (to_y, to_x)
            first_sem, second_sem = (x_sem, y_sem) if kind == 0 else (y_sem, x_sem)
            flip_x = (1 - x, x) if kind == 0 else (x, 1 - x)
            flip_y = (y, 1 - y) if kind == 0 else (1 - y, y)
            if 1 <= step < depth:
                zz = nearest(z, depth, step)
                piece = index(y, zz, x, core, kind)
                arrive(piece)
                onward = jnp.where(zz > z, z - 1, z + 1)

                @pl.when(jnp.logical_and(onward >= 0, onward < depth))
                def _():
                    send(downs.at[piece], piece, device(y, onward, x), line_sem.at[kind, zz])

                send(downs.at[piece], piece, first, first_sem)
                send(downs.at[piece], piece, second, second_sem)
                hand_over(piece)
            if 1 <= step <= depth:
                zz = nearest(z, depth, step - 1)
                piece = index(flip_y[0], zz, flip_x[0], core, kind)
                arrive(piece)
                send(downs.at[piece], piece, second, second_sem)
                hand_over(piece)
        for kind in range(kinds):
            flip_x = (1 - x, x) if kind == 0 else (x, 1 - x)
            flip_y = (y, 1 - y) if kind == 0 else (1 - y, y)
            if 1 <= step <= depth:
                zz = nearest(z, depth, step - 1)
                piece = index(flip_y[1], zz, flip_x[1], core, kind)
                arrive(piece)
                hand_over(piece)
            if 2 <= step <= depth + 1:
                zz = nearest(z, depth, step - 2)
                piece = index(1 - y, zz, 1 - x, core, kind)
                arrive(piece)
                hand_over(piece)
        if step == 2:
            weight_copy.wait()
            for j in range(train):
                @pl.when(t * train + j != group)
                def _():
                    pltpu.make_async_copy(ups.at[j], ups.at[j], up_recv.at[j]).wait()

                @pl.when(t * train + j == group)
                def _():
                    ups[j] = up_ref[...]
        if step >= 3:
            merge(step - 3)

    for kind in range(kinds):
        for zz in range(depth):
            onward = jnp.where(zz > z, z - 1, z + 1)

            @pl.when(jnp.logical_and(zz != z, jnp.logical_and(onward >= 0, onward < depth)))
            def _():
                pltpu.make_async_copy(downs.at[0], downs.at[0], line_sem.at[kind, zz]).wait()

        @pl.when(z > 0)
        def _():
            pltpu.make_async_copy(downs.at[0], downs.at[0], line_sem.at[kind, z]).wait()

        @pl.when(z < depth - 1)
        def _():
            pltpu.make_async_copy(downs.at[0], downs.at[0], line_sem.at[kind, depth]).wait()

    over_link = downs.at[pl.ds(0, 3 * depth)]
    pltpu.make_async_copy(over_link, over_link, x_sem).wait()
    pltpu.make_async_copy(over_link, over_link, y_sem).wait()
    handed = downs.at[pl.ds(0, kinds * (4 * depth - 1))]
    pltpu.make_async_copy(handed, handed, pass_sem).wait()
    for yy in range(train):
        @pl.when(yy * tp + up_target != group)
        def _():
            up_copy(yy).wait_send()


def relayed(tp, train, down, up, weight):
    layers, kinds, rank, columns = down.shape
    holders = tp * train
    kernel = functools.partial(gather_merge, tp, train, layers, kinds)
    vmem = pl.BlockSpec(memory_space=pltpu.VMEM)
    return pl.pallas_call(
        kernel,
        out_shape=pltpu.VMEM(weight.shape, weight.dtype),
        in_specs=[vmem, vmem, pl.BlockSpec(memory_space=pl.ANY)],
        out_specs=vmem,
        scratch_shapes=[
            pltpu.VMEM((holders * layers * kinds, rank, columns), down.dtype),
            pltpu.VMEM((train,) + up.shape, up.dtype),
            pltpu.SemaphoreType.DMA((holders * kinds,)),
            pltpu.SemaphoreType.DMA((holders * kinds,)),
            pltpu.SemaphoreType.DMA((2,)),
            pltpu.SemaphoreType.DMA((kinds, tp // 2 + 1)),
            pltpu.SemaphoreType.DMA,
            pltpu.SemaphoreType.DMA((train,)),
            pltpu.SemaphoreType.DMA((train,)),
            pltpu.SemaphoreType.DMA,
        ],
        compiler_params=pltpu.CompilerParams(
            collective_id=0, has_side_effects=True, vmem_limit_bytes=40 * 1024 * 1024
        ),
        name="gather_merge",
    )(down, up, weight)


def gathered(down, up, weight):
    per_rows = weight.shape[2]
    all_up = lax.all_gather(up, ("train", "tp"), axis=2, tiled=True)
    rows = lax.dynamic_slice_in_dim(all_up, lax.axis_index("tp") * per_rows, per_rows, 2)
    update = jnp.einsum(
        "eitd,eidh->eith",
        rows,
        lax.all_gather(down, ("train", "tp"), axis=3, tiled=True),
        preferred_element_type=jnp.float32,
    )
    return (weight.astype(jnp.float32) + adapter_scale * update).astype(jnp.bfloat16)


def per_device(tp, train, dp, down, up, weight):
    layers, kinds = down.shape[:2]
    if train == 2 and tp % 2 == 0 and tp >= 4 and layers == dp == 2 and kinds == 2:
        return relayed(tp, train, down, up, weight)
    return gathered(down, up, weight)


def solution(mesh):
    in_specs = (
        P(None, None, None, ("train", "tp")),
        P(None, None, ("train", "tp"), None),
        P(None, None, "tp", None),
    )
    out_specs = P(None, None, "tp", None)
    sizes = [mesh.shape[axis] for axis in ("tp", "train", "dp")]
    return jax.shard_map(
        functools.partial(per_device, *sizes),
        mesh=mesh, in_specs=in_specs, out_specs=out_specs, check_vma=False,
    )
```

```python
import functools

import jax
import jax.numpy as jnp
from jax import lax
from jax.experimental import pallas as pl
from jax.experimental.pallas import tpu as pltpu
from jax.sharding import PartitionSpec as P

adapter_scale = 2.0
MESH = pl.DeviceIdType.MESH


def place(train, tp, dp):
    return {"train": train, "tp": tp, "dp": dp}


def nearest(z, depth, j):
    if j == 0:
        return z
    low = jnp.minimum(z, depth - 1 - z)
    side = jnp.where(2 * z < depth - 1, 1, -1)
    near = z + side * ((j + 1) // 2) * (1 if j % 2 else -1)
    far = z + side * (j - low)
    return jnp.where(j <= 2 * low, near, far)


def gather_merge(
    tp, train, layers, kinds,
    down_ref, up_ref, weight_ref, out_ref,
    downs, ups, scaled, recv_sem, pass_recv, link_sem, line_sem, pass_sem, up_send, up_recv, weight_sem,
):
    y = lax.axis_index("train")
    t = lax.axis_index("tp")
    core = lax.axis_index("dp")
    depth = tp // 2
    z, x = t // 2, t % 2
    columns = down_ref.shape[-1]
    up_rows = up_ref.shape[2]
    other = 1 - core

    weight_copy = pltpu.make_async_copy(weight_ref, out_ref, weight_sem)
    weight_copy.start()

    def device(yy, zz, xx):
        return place(yy, zz * 2 + xx, core)

    to_x = device(y, z, 1 - x)
    to_y = device(1 - y, z, x)
    partner = place(y, t, other)

    group = y * tp + t
    up_target = group // train
    up_slot = group % train

    barrier = pltpu.get_barrier_semaphore()

    def greet(where):
        pl.semaphore_signal(barrier, inc=1, device_id=where, device_id_type=MESH)

    greet(to_x)
    greet(to_y)
    greet(partner)

    @pl.when(z > 0)
    def _():
        greet(device(y, z - 1, x))

    @pl.when(z < depth - 1)
    def _():
        greet(device(y, z + 1, x))

    for j in range(train):
        source = t * train + j

        @pl.when(source != group)
        def _():
            greet(place(source // tp, source % tp, core))

    peers = 3 + jnp.where(z > 0, 1, 0) + jnp.where(z < depth - 1, 1, 0)
    for yy in range(train):
        peers += jnp.where(yy * tp + up_target != group, 1, 0)
    pl.semaphore_wait(barrier, peers)

    def up_copy(yy):
        return pltpu.make_async_remote_copy(
            src_ref=up_ref, dst_ref=ups.at[up_slot],
            send_sem=up_send.at[yy], recv_sem=up_recv.at[up_slot],
            device_id=place(yy, up_target, core), device_id_type=MESH,
        )

    def index(yy, zz, xx, e, kind):
        return ((yy * tp + zz * 2 + xx) * layers + e) * kinds + kind

    def send(src, piece, where, sem):
        pltpu.make_async_remote_copy(
            src_ref=src, dst_ref=downs.at[piece], send_sem=sem,
            recv_sem=recv_sem.at[piece // (layers * kinds) * kinds + piece % kinds],
            device_id=where, device_id_type=MESH,
        ).start()

    def hand_over(piece):
        pltpu.make_async_remote_copy(
            src_ref=downs.at[piece], dst_ref=downs.at[piece], send_sem=pass_sem,
            recv_sem=pass_recv.at[piece // (layers * kinds) * kinds + piece % kinds],
            device_id=partner, device_id_type=MESH,
        ).start()

    def arrive(piece):
        sem = recv_sem.at[piece // (layers * kinds) * kinds + piece % kinds]
        pltpu.make_async_copy(downs.at[piece], downs.at[piece], sem).wait()

    x_sem, y_sem = link_sem.at[0], link_sem.at[1]

    for kind in range(kinds):
        piece = index(y, z, x, core, kind)
        mine = down_ref.at[core, kind]

        @pl.when(z > 0)
        def _():
            send(mine, piece, device(y, z - 1, x), line_sem.at[kind, z])

        @pl.when(z < depth - 1)
        def _():
            send(mine, piece, device(y, z + 1, x), line_sem.at[kind, depth])

        send(mine, piece, to_x, x_sem)
        send(mine, piece, to_y, y_sem)

    for yy in range(train):
        @pl.when(yy * tp + up_target != group)
        def _():
            up_copy(yy).start()

    for e in range(layers):
        for kind in range(kinds):
            downs[index(y, z, x, e, kind)] = down_ref[e, kind]

    def combine(yy, zz, xx, e, kind):
        block = downs[index(yy, zz, xx, e, kind)]
        at = pl.ds(pl.multiple_of((yy * tp + zz * 2 + xx) * columns, columns), columns)
        update = jnp.dot(
            scaled[e, kind], block, preferred_element_type=jnp.float32
        )
        old = out_ref[e, kind, :, at].astype(jnp.float32)
        out_ref[e, kind, :, at] = (old + update).astype(out_ref.dtype)

    def merge(level):
        zz = nearest(z, depth, level)
        for yy in (y, 1 - y):
            for xx in (x, 1 - x):
                if level == 0 and yy is y and xx is x:
                    continue
                for kind in range(kinds):
                    piece = index(yy, zz, xx, other, kind)
                    sem = pass_recv.at[piece // (layers * kinds) * kinds + piece % kinds]
                    pltpu.make_async_copy(downs.at[piece], downs.at[piece], sem).wait()

        def step(i, carry):
            kind = i % kinds
            e = i // kinds % layers
            corner = i // (kinds * layers)
            combine(corner // 2, zz, corner % 2, e, kind)
            return carry

        lax.fori_loop(0, 4 * layers * kinds, step, 0, unroll=4)

    for step in range(depth + 3):
        for kind in range(kinds):
            first, second = (to_x, to_y) if kind == 0 else (to_y, to_x)
            first_sem, second_sem = (x_sem, y_sem) if kind == 0 else (y_sem, x_sem)
            flip_x = (1 - x, x) if kind == 0 else (x, 1 - x)
            flip_y = (y, 1 - y) if kind == 0 else (1 - y, y)
            if 1 <= step < depth:
                zz = nearest(z, depth, step)
                piece = index(y, zz, x, core, kind)
                arrive(piece)
                onward = jnp.where(zz > z, z - 1, z + 1)

                @pl.when(jnp.logical_and(onward >= 0, onward < depth))
                def _():
                    send(downs.at[piece], piece, device(y, onward, x), line_sem.at[kind, zz])

                send(downs.at[piece], piece, first, first_sem)
                send(downs.at[piece], piece, second, second_sem)
                hand_over(piece)
            if 1 <= step <= depth:
                zz = nearest(z, depth, step - 1)
                piece = index(flip_y[0], zz, flip_x[0], core, kind)
                arrive(piece)
                send(downs.at[piece], piece, second, second_sem)
                hand_over(piece)
        for kind in range(kinds):
            flip_x = (1 - x, x) if kind == 0 else (x, 1 - x)
            flip_y = (y, 1 - y) if kind == 0 else (1 - y, y)
            if 1 <= step <= depth:
                zz = nearest(z, depth, step - 1)
                piece = index(flip_y[1], zz, flip_x[1], core, kind)
                arrive(piece)
                hand_over(piece)
            if 2 <= step <= depth + 1:
                zz = nearest(z, depth, step - 2)
                piece = index(1 - y, zz, 1 - x, core, kind)
                arrive(piece)
                hand_over(piece)
        if step == 2:
            weight_copy.wait()
            for j in range(train):
                @pl.when(t * train + j != group)
                def _():
                    pltpu.make_async_copy(ups.at[j], ups.at[j], up_recv.at[j]).wait()

                @pl.when(t * train + j == group)
                def _():
                    ups[j] = up_ref[...]

                scaled[:, :, pl.ds(j * up_rows, up_rows)] = ups[j] * adapter_scale
        if step >= 3:
            merge(step - 3)

    for kind in range(kinds):
        for zz in range(depth):
            onward = jnp.where(zz > z, z - 1, z + 1)

            @pl.when(jnp.logical_and(zz != z, jnp.logical_and(onward >= 0, onward < depth)))
            def _():
                pltpu.make_async_copy(downs.at[0], downs.at[0], line_sem.at[kind, zz]).wait()

        @pl.when(z > 0)
        def _():
            pltpu.make_async_copy(downs.at[0], downs.at[0], line_sem.at[kind, z]).wait()

        @pl.when(z < depth - 1)
        def _():
            pltpu.make_async_copy(downs.at[0], downs.at[0], line_sem.at[kind, depth]).wait()

    over_link = downs.at[pl.ds(0, 3 * depth)]
    pltpu.make_async_copy(over_link, over_link, x_sem).wait()
    pltpu.make_async_copy(over_link, over_link, y_sem).wait()
    handed = downs.at[pl.ds(0, kinds * (4 * depth - 1))]
    pltpu.make_async_copy(handed, handed, pass_sem).wait()
    for yy in range(train):
        @pl.when(yy * tp + up_target != group)
        def _():
            up_copy(yy).wait_send()


def relayed(tp, train, down, up, weight):
    layers, kinds, rank, columns = down.shape
    holders = tp * train
    kernel = functools.partial(gather_merge, tp, train, layers, kinds)
    vmem = pl.BlockSpec(memory_space=pltpu.VMEM)
    return pl.pallas_call(
        kernel,
        out_shape=pltpu.VMEM(weight.shape, weight.dtype),
        in_specs=[vmem, vmem, pl.BlockSpec(memory_space=pl.ANY)],
        out_specs=vmem,
        scratch_shapes=[
            pltpu.VMEM((holders * layers * kinds, rank, columns), down.dtype),
            pltpu.VMEM((train,) + up.shape, up.dtype),
            pltpu.VMEM(weight.shape[:3] + (rank,), up.dtype),
            pltpu.SemaphoreType.DMA((holders * kinds,)),
            pltpu.SemaphoreType.DMA((holders * kinds,)),
            pltpu.SemaphoreType.DMA((2,)),
            pltpu.SemaphoreType.DMA((kinds, tp // 2 + 1)),
            pltpu.SemaphoreType.DMA,
            pltpu.SemaphoreType.DMA((train,)),
            pltpu.SemaphoreType.DMA((train,)),
            pltpu.SemaphoreType.DMA,
        ],
        compiler_params=pltpu.CompilerParams(
            collective_id=0, has_side_effects=True, vmem_limit_bytes=40 * 1024 * 1024
        ),
        name="gather_merge",
    )(down, up, weight)


def gathered(down, up, weight):
    per_rows = weight.shape[2]
    all_up = lax.all_gather(up, ("train", "tp"), axis=2, tiled=True)
    rows = lax.dynamic_slice_in_dim(all_up, lax.axis_index("tp") * per_rows, per_rows, 2)
    update = jnp.einsum(
        "eitd,eidh->eith",
        rows,
        lax.all_gather(down, ("train", "tp"), axis=3, tiled=True),
        preferred_element_type=jnp.float32,
    )
    return (weight.astype(jnp.float32) + adapter_scale * update).astype(jnp.bfloat16)


def per_device(tp, train, dp, down, up, weight):
    layers, kinds = down.shape[:2]
    if train == 2 and tp % 2 == 0 and tp >= 4 and layers == dp == 2 and kinds == 2:
        return relayed(tp, train, down, up, weight)
    return gathered(down, up, weight)


def solution(mesh):
    in_specs = (
        P(None, None, None, ("train", "tp")),
        P(None, None, ("train", "tp"), None),
        P(None, None, "tp", None),
    )
    out_specs = P(None, None, "tp", None)
    sizes = [mesh.shape[axis] for axis in ("tp", "train", "dp")]
    return jax.shard_map(
        functools.partial(per_device, *sizes),
        mesh=mesh, in_specs=in_specs, out_specs=out_specs, check_vma=False,
    )
```
